8 devices in a mesh: replica: 1 (over z), data2: 2 (over y), data: 4 (over x, core).
Axes of the slice: x: 2, y: 2, z: 1, core: 2. Of those that a mesh axis runs over, the one named last changes fastest.
Arguments:
- q_hidden: bfloat16 [16, 32, 768], P(('replica', 'data2', 'data'))
- d_hidden: bfloat16 [16, 8192, 768], P(('replica', 'data2', 'data'))
- w_proj: bfloat16 [768, 128], replicated
- q_mask: int32 [16, 32], P(('replica', 'data2', 'data'))
- d_mask: int32 [16, 8192], P(('replica', 'data2', 'data'))
- temperature: float32 [], replicated
Outputs:
- output 1: float32 [16], P(('replica', 'data2', 'data'))
- output 2: float32 [1], P('replica')
All inputs are finite; a program needn't handle non-finite values.
Results may differ from the reference program's by a relative error of at most 0.00163984.
Values are sent between devices in bfloat16 or wider.
A program may use at most 1 GiB of HBM per device.

```python
import math
import jax
import jax.numpy as jnp
from jax import lax

BATCH = 16
QLEN = 32
DLEN = 8192
HIDDEN = 768
PROJ = 128

NORM_EPS = 1e-6
TAU_SCALE = QLEN / (8.0 * math.log(BATCH))


def setup_inputs(seed: int = 0, part: int = 0) -> dict:
    base_key = jax.random.key(seed)
    rand_keys = jax.random.split(jax.random.fold_in(base_key, part), 7)
    shared = jax.random.normal(rand_keys[0], (HIDDEN,), jnp.float32)
    doc_len = jax.random.randint(rand_keys[1], (BATCH,), DLEN // 2, DLEN + 1)
    qry_len = jax.random.randint(rand_keys[2], (BATCH,), QLEN // 2, QLEN + 1)
    doc_mask = (jnp.arange(DLEN)[None, :] < doc_len[:, None]).astype(jnp.int32)
    qry_mask = (jnp.arange(QLEN)[None, :] < qry_len[:, None]).astype(jnp.int32)
    doc_noise = jax.random.normal(rand_keys[3], (BATCH, DLEN, HIDDEN), jnp.float32)
    src_pos = jax.random.randint(rand_keys[4], (BATCH, QLEN), 0, doc_len[:, None])
    src_idx = jnp.broadcast_to(src_pos[:, :, None], (BATCH, QLEN, HIDDEN))
    copied = jnp.take_along_axis(doc_noise, src_idx, axis=1)
    share_w = jax.random.uniform(rand_keys[5], (BATCH, 1, 1), jnp.float32, 0.15, 0.4)
    fresh = jax.random.normal(rand_keys[6], (BATCH, QLEN, HIDDEN), jnp.float32)
    half_amp = math.sqrt(0.5)
    d_keep = doc_mask[:, :, None] > 0
    d_hidden = jnp.where(d_keep, half_amp, 2.0) * shared + jnp.where(d_keep, half_amp, 0.3) * doc_noise
    q_keep = qry_mask[:, :, None] > 0
    q_mix = jnp.sqrt(share_w) * copied + jnp.sqrt(1.0 - share_w) * fresh
    q_body = jnp.where(q_keep, q_mix, copied)
    q_hidden = jnp.where(q_keep, 1.0, 2.5) * (half_amp * shared + half_amp * q_body)
    w_proj = jax.random.normal(jax.random.fold_in(base_key, 1000), (HIDDEN, PROJ), jnp.float32) * HIDDEN ** -0.5
    temperature = jax.random.uniform(jax.random.fold_in(base_key, 2000), (), jnp.float32, 0.6, 1.4) * TAU_SCALE
    return {
        'q_hidden': q_hidden.astype(jnp.bfloat16),
        'd_hidden': d_hidden.astype(jnp.bfloat16),
        'w_proj': w_proj.astype(jnp.bfloat16),
        'q_mask': qry_mask,
        'd_mask': doc_mask,
        'temperature': temperature.astype(jnp.float32),
    }


def project(hidden, w_proj):
    flat_rows = hidden.reshape(-1, hidden.shape[-1])
    proj_f32 = jnp.dot(flat_rows, w_proj, preferred_element_type=jnp.float32)
    row_norm = jnp.sqrt(jnp.sum(proj_f32 * proj_f32, axis=-1, keepdims=True) + NORM_EPS)
    unit_rows = (proj_f32 / row_norm).astype(jnp.bfloat16)
    return unit_rows.reshape(hidden.shape[:-1] + (w_proj.shape[1],))


def reference(q_hidden, d_hidden, w_proj, q_mask, d_mask, temperature):
    q_tok = project(q_hidden, w_proj).astype(jnp.float32)
    d_tok = project(d_hidden, w_proj).astype(jnp.float32)
    d_valid = d_mask > 0
    q_weight = q_mask.astype(jnp.float32)

    def score_row(row_in):
        q_row, weight_row = row_in
        sim_vals = jnp.einsum('td,psd->tps', q_row, d_tok)
        best_sim = jnp.max(jnp.where(d_valid[None], sim_vals, -jnp.inf), axis=-1)
        return jnp.sum(weight_row[:, None] * best_sim, axis=0)

    scores = lax.map(score_row, (q_tok, q_weight))
    logits = scores / temperature
    row_max = jnp.max(logits, axis=1, keepdims=True)
    log_norm = row_max[:, 0] + jnp.log(jnp.sum(jnp.exp(logits - row_max), axis=1))
    loss_rows = log_norm - jnp.diagonal(logits)
    return loss_rows, jnp.mean(loss_rows).reshape(1)
```

```python
import functools

import jax
import jax.numpy as jnp
from jax import lax
from jax.experimental import pallas as pl
from jax.experimental.pallas import tpu as pltpu
from jax.sharding import PartitionSpec as P

NORM_EPS = 1e-6
ROW_AXES = ('replica', 'data2', 'data')
BLOCK = 1024
LAG = 8
NEG = float('-inf')


def kernel(sizes, q_hbm, d_hbm, w_hbm, qm_ref, dm_ref, temp_ref, rows_ref, mean_ref,
           h_ref, q_ref, w_ref, wt_ref, et_ref, qall_ref, best_ref, sall_ref,
           in_sem, h_sem, q_send, q_recv, s_send, s_recv):
    outer, inner, per_dev, q_len, d_len, hidden, proj = sizes
    group = outer * inner
    n_blocks = per_dev * d_len // BLOCK
    doc_blocks = d_len // BLOCK
    d2 = lax.axis_index('data2')
    d1 = lax.axis_index('data')
    me = d2 * inner + d1

    def peer(step):
        other = lax.rem(me + step, group)
        return other, {'data2': other // inner, 'data': lax.rem(other, inner)}

    w_copy = pltpu.make_async_copy(w_hbm, w_ref, in_sem.at[0])
    q_copy = pltpu.make_async_copy(q_hbm, q_ref, in_sem.at[1])
    w_copy.start()
    q_copy.start()

    def h_copy(block):
        return pltpu.make_async_copy(
            d_hbm.at[pl.ds(block * BLOCK, BLOCK)], h_ref.at[pl.ds(block * BLOCK, BLOCK)], h_sem.at[block])

    for block in range(n_blocks):
        h_copy(block).start()

    barrier = pltpu.get_barrier_semaphore()
    for step in range(1, group):
        pl.semaphore_signal(barrier, inc=1, device_id=peer(step)[1], device_id_type=pl.DeviceIdType.MESH)

    w_copy.wait()
    q_copy.wait()
    y = jnp.dot(q_ref[...], w_ref[...], preferred_element_type=jnp.float32)
    unit = y * lax.rsqrt(jnp.sum(y * y, axis=1, keepdims=True) + NORM_EPS)
    eye = lax.broadcasted_iota(jnp.int32, (q_len, q_len), 0) == lax.broadcasted_iota(jnp.int32, (q_len, q_len), 1)
    for i in range(per_dev):
        keep = jnp.sum(jnp.where(eye, qm_ref[pl.ds(i, 1), :], 0), axis=1, keepdims=True)
        rows = jnp.where(keep > 0, unit[i * q_len:(i + 1) * q_len], 0.0)
        qall_ref[me, pl.ds(i * q_len, q_len), :] = rows.astype(jnp.bfloat16)
    wt_ref[...] = jnp.transpose(w_ref[...], (1, 0))

    pl.semaphore_wait(barrier, group - 1)

    def q_copy_to(step):
        return pltpu.make_async_remote_copy(
            src_ref=qall_ref.at[me], dst_ref=qall_ref.at[me], send_sem=q_send.at[step], recv_sem=q_recv.at[me],
            device_id=peer(step)[1], device_id_type=pl.DeviceIdType.MESH)

    for step in range(1, group):
        q_copy_to(step).start()

    best_ref[...] = jnp.full(best_ref.shape, NEG, jnp.float32)

    def project(block):
        h_copy(block).wait()
        h = h_ref[pl.ds(block * BLOCK, BLOCK), :]
        y = lax.dot_general(wt_ref[...], h, (((1,), (1,)), ((), ())), preferred_element_type=jnp.float32)
        inv = lax.rsqrt(jnp.sum(y * y, axis=0, keepdims=True) + NORM_EPS)
        et_ref[block] = (y * inv).astype(jnp.bfloat16)

    def score(block):
        doc = block // doc_blocks
        col = lax.rem(block, doc_blocks) * BLOCK
        q = qall_ref[...].reshape(group * per_dev * q_len, proj)
        for t in range(0, BLOCK, 512):
            s = jnp.dot(q, et_ref[block, :, t:t + 512], preferred_element_type=jnp.float32)
            valid = dm_ref[pl.ds(doc, 1), pl.ds(pl.multiple_of(col + t, 128), 512)] > 0
            s = s + jnp.where(valid, 0.0, NEG)
            m = jnp.maximum(jnp.maximum(s[:, :128], s[:, 128:256]), jnp.maximum(s[:, 256:384], s[:, 384:]))
            best_ref[doc] = jnp.maximum(best_ref[doc], m)

    def loop(lo, hi, body):
        def step(i, carry):
            body(i)
            return carry
        lax.fori_loop(lo, hi, step, 0)

    loop(0, LAG, project)

    for step in range(1, group):
        other = lax.rem(me + step, group)
        pltpu.make_async_remote_copy(
            src_ref=qall_ref.at[other], dst_ref=qall_ref.at[other], send_sem=q_send.at[step],
            recv_sem=q_recv.at[other], device_id=peer(step)[1], device_id_type=pl.DeviceIdType.MESH).wait_recv()

    def both(block):
        project(block)
        score(block - LAG)

    loop(LAG, n_blocks, both)
    loop(n_blocks - LAG, n_blocks, score)

    n_rows = group * per_dev
    lane = lax.broadcasted_iota(jnp.int32, (n_rows, 128), 1)
    mine = jnp.zeros((n_rows, 128), jnp.float32)
    for d in range(per_dev):
        m = jnp.max(best_ref[d], axis=1, keepdims=True)
        m = jnp.broadcast_to(m, (n_rows * q_len, 128)).reshape(n_rows, q_len, 128)
        mine = jnp.where(lane == me * per_dev + d, jnp.sum(m, axis=1), mine)
    sall_ref[me] = mine

    def s_copy_to(step):
        return pltpu.make_async_remote_copy(
            src_ref=sall_ref.at[me], dst_ref=sall_ref.at[me], send_sem=s_send.at[step], recv_sem=s_recv.at[me],
            device_id=peer(step)[1], device_id_type=pl.DeviceIdType.MESH)

    for step in range(1, group):
        s_copy_to(step).start()
    for step in range(1, group):
        q_copy_to(step).wait_send()
    for step in range(1, group):
        other = lax.rem(me + step, group)
        pltpu.make_async_remote_copy(
            src_ref=sall_ref.at[other], dst_ref=sall_ref.at[other], send_sem=s_send.at[step],
            recv_sem=s_recv.at[other], device_id=peer(step)[1], device_id_type=pl.DeviceIdType.MESH).wait_recv()

    total = sall_ref[0]
    for d in range(1, group):
        total = total + sall_ref[d]
    logits = total / temp_ref[0]
    logits = jnp.where(lane < n_rows, logits, NEG)
    top = jnp.max(logits, axis=1, keepdims=True)
    log_norm = top + jnp.log(jnp.sum(jnp.exp(logits - top), axis=1, keepdims=True))
    row = lax.broadcasted_iota(jnp.int32, (n_rows, 128), 0)
    own = jnp.sum(jnp.where(row == lane, logits, 0.0), axis=1, keepdims=True)
    loss = jnp.broadcast_to(log_norm - own, (n_rows, 128))
    mean_ref[...] = jnp.sum(loss, axis=0, keepdims=True)[:, :1] / n_rows
    picked = jnp.sum(jnp.where(row == lane + me * per_dev, loss, 0.0), axis=0, keepdims=True)
    rows_ref[...] = picked[:, :per_dev]
    for step in range(1, group):
        s_copy_to(step).wait_send()


def solution(mesh):
    outer = mesh.shape['data2']
    inner = mesh.shape['data']
    group = outer * inner

    def device_fn(q_hidden, d_hidden, w_proj, q_mask, d_mask, value_a11):
        per_dev, q_len, hidden = q_hidden.shape
        d_len = d_hidden.shape[1]
        proj = w_proj.shape[1]
        sizes = (outer, inner, per_dev, q_len, d_len, hidden, proj)
        n_tok = per_dev * d_len
        n_blocks = n_tok // BLOCK
        n_rows = group * per_dev
        any_spec = pl.BlockSpec(memory_space=pl.ANY)
        vmem_spec = pl.BlockSpec(memory_space=pltpu.VMEM)
        rows, mean = pl.pallas_call(
            functools.partial(kernel, sizes),
            out_shape=(jax.ShapeDtypeStruct((1, per_dev), jnp.float32), jax.ShapeDtypeStruct((1, 1), jnp.float32)),
            in_specs=[any_spec, any_spec, any_spec, vmem_spec, vmem_spec, pl.BlockSpec(memory_space=pltpu.SMEM)],
            out_specs=(vmem_spec, vmem_spec),
            scratch_shapes=[
                pltpu.VMEM((n_tok, hidden), jnp.bfloat16),
                pltpu.VMEM((per_dev * q_len, hidden), jnp.bfloat16),
                pltpu.VMEM((hidden, proj), jnp.bfloat16),
                pltpu.VMEM((proj, hidden), jnp.bfloat16),
                pltpu.VMEM((n_blocks, proj, BLOCK), jnp.bfloat16),
                pltpu.VMEM((group, per_dev * q_len, proj), jnp.bfloat16),
                pltpu.VMEM((per_dev, n_rows * q_len, 128), jnp.float32),
                pltpu.VMEM((group, n_rows, 128), jnp.float32),
                pltpu.SemaphoreType.DMA((2,)),
                pltpu.SemaphoreType.DMA((n_blocks,)),
                pltpu.SemaphoreType.DMA((group,)),
                pltpu.SemaphoreType.DMA((group,)),
                pltpu.SemaphoreType.DMA((group,)),
                pltpu.SemaphoreType.DMA((group,)),
            ],
            compiler_params=pltpu.CompilerParams(
                collective_id=0, has_side_effects=True, vmem_limit_bytes=60 * 1024 * 1024),
            name='colbert_loss',
        )(q_hidden.reshape(per_dev * q_len, hidden), d_hidden.reshape(n_tok, hidden), w_proj, q_mask, d_mask,
          value_a11.reshape(1))
        return rows.reshape(per_dev), mean.reshape(1)

    return jax.shard_map(
        device_fn,
        mesh=mesh,
        in_specs=(P(ROW_AXES), P(ROW_AXES), P(), P(ROW_AXES), P(ROW_AXES), P()),
        out_specs=(P(ROW_AXES), P('replica')),
        check_vma=False,
    )
```

```python
import functools

import jax
import jax.numpy as jnp
from jax import lax
from jax.experimental import pallas as pl
from jax.experimental.pallas import tpu as pltpu
from jax.sharding import PartitionSpec as P

NORM_EPS = 1e-6
ROW_AXES = ('replica', 'data2', 'data')
TILE = 256
STEP = 2 * TILE
CHUNK = 1024
LAG = 12
PIECE = 128
MASKED = -1e30
MESH = pl.DeviceIdType.MESH


def kernel(sizes, q_hbm, d_hbm, w_hbm, qm_hbm, dm_hbm, temp_hbm, rows_ref, mean_ref,
           h_ref, q_ref, w_ref, wt_ref, qm_ref, dm_ref, temp_ref, et_ref, qall_ref, best_ref, part_ref, sall_ref,
           in_sem, h_sem, q_send, q_recv, s_send, s_recv):
    outer, inner, per_dev, q_len, d_len, hidden, proj = sizes
    group = outer * inner
    n_rows = group * per_dev
    n_tok = per_dev * d_len
    n_chunks = n_tok // CHUNK
    n_steps = n_tok // STEP
    doc_steps = d_len // STEP
    k_tiles = hidden // TILE
    pieces = n_rows * q_len // PIECE
    q_rows = per_dev * q_len
    d2 = lax.axis_index('data2')
    d1 = lax.axis_index('data')
    me = d2 * inner + d1

    def peer(step):
        other = lax.rem(me + step, group)
        return other, {'data2': other // inner, 'data': lax.rem(other, inner)}

    small = [pltpu.make_async_copy(src, dst, in_sem.at[i]) for i, (src, dst) in enumerate((
        (w_hbm, w_ref), (q_hbm, q_ref), (qm_hbm, qm_ref), (dm_hbm, dm_ref), (temp_hbm, temp_ref)))]
    for copy in small:
        copy.start()

    barrier = pltpu.get_barrier_semaphore()
    for step in range(1, group):
        pl.semaphore_signal(barrier, inc=1, device_id=peer(step)[1], device_id_type=MESH)

    def h_copy(chunk):
        rows = pl.ds(chunk * CHUNK, CHUNK)
        return pltpu.make_async_copy(d_hbm.at[rows], h_ref.at[rows], h_sem.at[chunk])

    for chunk in range(n_chunks):
        h_copy(chunk).start(priority=1)

    for copy in small[:3]:
        copy.wait()

    def project_queries():
        y = jnp.dot(q_ref[...], w_ref[...], preferred_element_type=jnp.float32)
        unit = y * lax.rsqrt(jnp.sum(y * y, axis=1, keepdims=True) + NORM_EPS)
        eye = (lax.broadcasted_iota(jnp.int32, (q_len, q_len), 0)
               == lax.broadcasted_iota(jnp.int32, (q_len, q_len), 1))
        for i in range(per_dev):
            keep = jnp.sum(jnp.where(eye, qm_ref[i:i + 1, :], 0), axis=1, keepdims=True)
            rows = jnp.where(keep > 0, unit[i * q_len:(i + 1) * q_len], 0.0)
            qall_ref[me, pl.ds(i * q_len, q_len), :] = rows.astype(jnp.bfloat16)

    project_queries()
    wt_ref[...] = jnp.transpose(w_ref[...], (1, 0))

    pl.semaphore_wait(barrier, group - 1)

    def q_copy(step, slot):
        return pltpu.make_async_remote_copy(
            src_ref=qall_ref.at[slot], dst_ref=qall_ref.at[slot], send_sem=q_send.at[step], recv_sem=q_recv.at[slot],
            device_id=peer(step)[1], device_id_type=MESH)

    def s_copy(step, slot):
        return pltpu.make_async_remote_copy(
            src_ref=sall_ref.at[slot], dst_ref=sall_ref.at[slot], send_sem=s_send.at[step], recv_sem=s_recv.at[slot],
            device_id=peer(step)[1], device_id_type=MESH)

    for step in range(1, group):
        q_copy(step, me).start()
    small[3].wait()

    def doc_part(doc):
        m = jnp.max(best_ref[doc], axis=1, keepdims=True)
        m = jnp.broadcast_to(m, (n_rows * q_len, 128)).reshape(n_rows, q_len, 128)
        return jnp.sum(m, axis=1)

    ones_col = jnp.where(lax.broadcasted_iota(jnp.int32, (n_rows * q_len, 128), 1) == 0, 1.0, 0.0).astype(jnp.bfloat16)
    top_row = lax.broadcasted_iota(jnp.int32, (16, STEP), 0) == 0

    def project(step):
        if step * STEP % CHUNK == 0:
            h_copy(step * STEP // CHUNK).wait()
        h = h_ref[step * STEP:(step + 1) * STEP, :]
        y = lax.dot_general(wt_ref[...], h, (((1,), (1,)), ((), ())), preferred_element_type=jnp.float32)
        inv = lax.rsqrt(jnp.sum(y * y, axis=0, keepdims=True) + NORM_EPS)
        et_ref[step, :proj, :] = (y * inv).astype(jnp.bfloat16)
        doc = step * STEP // d_len
        col = step * STEP % d_len
        valid = dm_ref[doc:doc + 1, col:col + STEP] > 0
        bias = jnp.where(top_row, jnp.where(valid, 0.0, MASKED), 0.0)
        et_ref[step, proj:, :] = bias.astype(jnp.bfloat16)

    def score(step):
        doc = step // doc_steps
        q = qall_ref[...].reshape(n_rows * q_len, proj)
        lhs = jnp.concatenate([q, ones_col], axis=1)
        rhs = jnp.concatenate([et_ref[step], jnp.zeros((TILE - proj - 16, STEP), jnp.bfloat16)], axis=0)
        s = jnp.dot(lhs, rhs, preferred_element_type=jnp.float32)
        m = jnp.maximum(jnp.maximum(s[:, :128], s[:, 128:256]), jnp.maximum(s[:, 256:384], s[:, 384:]))
        if step % doc_steps:
            m = jnp.maximum(m, best_ref[doc])
        best_ref[doc] = m

    for step in range(n_steps + LAG):
        if step == LAG:
            for peer_step in range(1, group):
                q_copy(peer_step, lax.rem(me + peer_step, group)).wait_recv()
        if step < n_steps:
            project(step)
        if step >= LAG:
            score(step - LAG)
        if step == LAG + doc_steps:
            part_ref[0] = doc_part(0)

    lane = lax.broadcasted_iota(jnp.int32, (n_rows, 128), 1)
    first = jnp.where(lane == me * per_dev, part_ref[0], 0.0)
    sall_ref[me] = jnp.where(lane == me * per_dev + 1, doc_part(1), first)

    for step in range(1, group):
        s_copy(step, me).start()
    small[4].wait()
    for step in range(1, group):
        q_copy(step, me).wait_send()
    for step in range(1, group):
        s_copy(step, lax.rem(me + step, group)).wait_recv()

    total = sall_ref[0]
    for d in range(1, group):
        total = total + sall_ref[d]
    logits = total / temp_ref[0]
    logits = jnp.where(lane < n_rows, logits, float('-inf'))
    top = jnp.max(logits, axis=1, keepdims=True)
    log_norm = top + jnp.log(jnp.sum(jnp.exp(logits - top), axis=1, keepdims=True))
    row = lax.broadcasted_iota(jnp.int32, (n_rows, 128), 0)
    own = jnp.sum(jnp.where(row == lane, logits, 0.0), axis=1, keepdims=True)
    loss = jnp.broadcast_to(log_norm - own, (n_rows, 128))
    mean_ref[...] = jnp.sum(loss, axis=0, keepdims=True)[:, :1] / n_rows
    picked = jnp.sum(jnp.where(row == lane + me * per_dev, loss, 0.0), axis=0, keepdims=True)
    rows_ref[...] = picked[:, :per_dev]
    for step in range(1, group):
        s_copy(step, me).wait_send()


def solution(mesh):
    outer = mesh.shape['data2']
    inner = mesh.shape['data']
    group = outer * inner

    def device_fn(q_hidden, d_hidden, w_proj, q_mask, d_mask, value_a11):
        per_dev, q_len, hidden = q_hidden.shape
        d_len = d_hidden.shape[1]
        proj = w_proj.shape[1]
        sizes = (outer, inner, per_dev, q_len, d_len, hidden, proj)
        n_tok = per_dev * d_len
        n_rows = group * per_dev
        any_spec = pl.BlockSpec(memory_space=pl.ANY)
        vmem_spec = pl.BlockSpec(memory_space=pltpu.VMEM)
        rows, mean = pl.pallas_call(
            functools.partial(kernel, sizes),
            out_shape=(jax.ShapeDtypeStruct((1, per_dev), jnp.float32), jax.ShapeDtypeStruct((1, 1), jnp.float32)),
            in_specs=[any_spec] * 6,
            out_specs=(vmem_spec, vmem_spec),
            scratch_shapes=[
                pltpu.VMEM((n_tok, hidden), jnp.bfloat16),
                pltpu.VMEM((per_dev * q_len, hidden), jnp.bfloat16),
                pltpu.VMEM((hidden, proj), jnp.bfloat16),
                pltpu.VMEM((proj, hidden), jnp.bfloat16),
                pltpu.VMEM((per_dev, q_len), jnp.int32),
                pltpu.VMEM((per_dev, d_len), jnp.int32),
                pltpu.SMEM((1,), jnp.float32),
                pltpu.VMEM((n_tok // STEP, proj + 16, STEP), jnp.bfloat16),
                pltpu.VMEM((group, per_dev * q_len, proj), jnp.bfloat16),
                pltpu.VMEM((per_dev, n_rows * q_len, 128), jnp.float32),
                pltpu.VMEM((1, n_rows, 128), jnp.float32),
                pltpu.VMEM((group, n_rows, 128), jnp.float32),
                pltpu.SemaphoreType.DMA((5,)),
                pltpu.SemaphoreType.DMA((n_tok // CHUNK,)),
                pltpu.SemaphoreType.DMA((group,)),
                pltpu.SemaphoreType.DMA((group,)),
                pltpu.SemaphoreType.DMA((group,)),
                pltpu.SemaphoreType.DMA((group,)),
            ],
            compiler_params=pltpu.CompilerParams(
                collective_id=0, has_side_effects=True, vmem_limit_bytes=60 * 1024 * 1024),
            name='colbert_loss',
        )(q_hidden.reshape(per_dev * q_len, hidden), d_hidden.reshape(n_tok, hidden), w_proj, q_mask, d_mask,
          value_a11.reshape(1))
        return rows.reshape(per_dev), mean.reshape(1)

    return jax.shard_map(
        device_fn,
        mesh=mesh,
        in_specs=(P(ROW_AXES), P(ROW_AXES), P(), P(ROW_AXES), P(ROW_AXES), P()),
        out_specs=(P(ROW_AXES), P('replica')),
        check_vma=False,
    )
```

```python
import functools

import jax
import jax.numpy as jnp
from jax import lax
from jax.experimental import pallas as pl
from jax.experimental.pallas import tpu as pltpu
from jax.sharding import PartitionSpec as P

NORM_EPS = 1e-6
ROW_AXES = ('replica', 'data2', 'data')
TILE = 256
STEP = 2 * TILE
CHUNKS = (2, 2, 4, 4, 4, 6, 10)
LAG = 12
PIECE = 256
MASKED = -1e30
MESH = pl.DeviceIdType.MESH


def kernel(sizes, q_hbm, d_hbm, w_hbm, qm_hbm, dm_hbm, out_ref,
           h_ref, q_ref, w_ref, wt_ref, qm_ref, dm_ref, et_ref, qall_ref, best_ref, sall_ref,
           in_sem, h_sem, q_send, q_recv, s_send, s_recv):
    outer, inner, per_dev, q_len, d_len, hidden, proj = sizes
    group = outer * inner
    n_rows = group * per_dev
    n_tok = per_dev * d_len
    starts = [sum(CHUNKS[:i]) for i in range(len(CHUNKS))]
    n_steps = n_tok // STEP
    doc_steps = d_len // STEP
    k_tiles = hidden // TILE
    pieces = n_rows * q_len // PIECE
    q_rows = per_dev * q_len
    d2 = lax.axis_index('data2')
    d1 = lax.axis_index('data')
    me = d2 * inner + d1

    def peer(step):
        other = lax.rem(me + step, group)
        return other, {'data2': other // inner, 'data': lax.rem(other, inner)}

    small = [pltpu.make_async_copy(src, dst, in_sem.at[i]) for i, (src, dst) in enumerate((
        (w_hbm, w_ref), (q_hbm, q_ref), (qm_hbm, qm_ref), (dm_hbm, dm_ref)))]
    for copy in small:
        copy.start()

    barrier = pltpu.get_barrier_semaphore()
    for step in range(1, group):
        pl.semaphore_signal(barrier, inc=1, device_id=peer(step)[1], device_id_type=MESH)

    def h_copy(chunk):
        rows = pl.ds(starts[chunk] * STEP, CHUNKS[chunk] * STEP)
        return pltpu.make_async_copy(d_hbm.at[rows], h_ref.at[rows], h_sem.at[chunk])

    for chunk in range(len(CHUNKS)):
        h_copy(chunk).start(priority=1)

    for copy in small[:3]:
        copy.wait()

    def project_queries():
        y = jnp.dot(q_ref[...], w_ref[...], preferred_element_type=jnp.float32)
        unit = y * lax.rsqrt(jnp.sum(y * y, axis=1, keepdims=True) + NORM_EPS)
        eye = (lax.broadcasted_iota(jnp.int32, (q_len, q_len), 0)
               == lax.broadcasted_iota(jnp.int32, (q_len, q_len), 1))
        for i in range(per_dev):
            keep = jnp.sum(jnp.where(eye, qm_ref[i:i + 1, :], 0), axis=1, keepdims=True)
            rows = jnp.where(keep > 0, unit[i * q_len:(i + 1) * q_len], 0.0)
            qall_ref[me, pl.ds(i * q_len, q_len), :] = rows.astype(jnp.bfloat16)

    project_queries()

    pl.semaphore_wait(barrier, group - 1)

    def q_copy(step, slot):
        return pltpu.make_async_remote_copy(
            src_ref=qall_ref.at[slot], dst_ref=qall_ref.at[slot], send_sem=q_send.at[step], recv_sem=q_recv.at[slot],
            device_id=peer(step)[1], device_id_type=MESH)

    def s_copy(step, slot):
        return pltpu.make_async_remote_copy(
            src_ref=sall_ref.at[slot], dst_ref=sall_ref.at[slot], send_sem=s_send.at[step], recv_sem=s_recv.at[slot],
            device_id=peer(step)[1], device_id_type=MESH)

    for step in range(1, group):
        q_copy(step, me).start()
    wt_ref[...] = jnp.transpose(w_ref[...], (1, 0))
    small[3].wait()

    def doc_row(doc):
        m = jnp.max(best_ref[doc], axis=1, keepdims=True)
        lane = lax.broadcasted_iota(jnp.int32, (n_rows * q_len, 128), 1)
        query = lax.broadcasted_iota(jnp.int32, (n_rows * q_len, 128), 0) // q_len
        return jnp.sum(jnp.where(lane == query, m, 0.0), axis=0, keepdims=True)

    ones_col = jnp.where(lax.broadcasted_iota(jnp.int32, (PIECE, 128), 1) == 0, 1.0, 0.0).astype(jnp.bfloat16)
    top_row = lax.broadcasted_iota(jnp.int32, (16, STEP), 0) == 0
    zeros = jnp.zeros((TILE - proj - 16, STEP), jnp.bfloat16)
    partial = {}

    def project(step, k):
        if k == 0 and step in starts and (step < LAG or step > LAG):
            h_copy(starts.index(step)).wait()
        h = h_ref[step * STEP:(step + 1) * STEP, k * TILE:(k + 1) * TILE]
        y = lax.dot_general(wt_ref[:, k * TILE:(k + 1) * TILE], h, (((1,), (1,)), ((), ())),
                            preferred_element_type=jnp.float32)
        if k:
            y = partial[step] + y
        partial[step] = y
        if k < k_tiles - 1:
            return
        del partial[step]
        inv = lax.rsqrt(jnp.sum(y * y, axis=0, keepdims=True) + NORM_EPS)
        et_ref[step, :proj, :] = (y * inv).astype(jnp.bfloat16)
        doc = step * STEP // d_len
        col = step * STEP % d_len
        valid = dm_ref[doc:doc + 1, col:col + STEP] > 0
        bias = jnp.where(top_row, jnp.where(valid, 0.0, MASKED), 0.0)
        et_ref[step, proj:, :] = bias.astype(jnp.bfloat16)

    def score(step, piece):
        doc = step // doc_steps
        per_piece = PIECE // q_rows
        q = qall_ref[piece * per_piece:(piece + 1) * per_piece].reshape(PIECE, proj)
        lhs = jnp.concatenate([q, ones_col], axis=1)
        rhs = jnp.concatenate([et_ref[step], zeros], axis=0)
        s = jnp.dot(lhs, rhs, preferred_element_type=jnp.float32)
        m = jnp.maximum(jnp.maximum(s[:, :128], s[:, 128:256]), jnp.maximum(s[:, 256:384], s[:, 384:]))
        rows = pl.ds(piece * PIECE, PIECE)
        if step % doc_steps:
            m = jnp.maximum(m, best_ref[doc, rows, :])
        best_ref[doc, rows, :] = m
        if step == doc_steps - 1 and piece == pieces - 1:
            sall_ref[me, 0:1, :] = doc_row(0)

    projects = [(step, k) for step in range(n_steps) for k in range(k_tiles)]
    scores = [(step, piece) for step in range(n_steps) for piece in range(pieces)]
    for item in projects[:LAG * k_tiles]:
        project(*item)
    projects = projects[LAG * k_tiles:]
    for peer_step in range(1, group):
        q_copy(peer_step, lax.rem(me + peer_step, group)).wait_recv()
    if LAG in starts:
        h_copy(starts.index(LAG)).wait()
    while scores:
        score(*scores.pop(0))
        if projects:
            project(*projects.pop(0))

    sall_ref[me, 1:2, :] = doc_row(1)
    for step in range(1, group):
        s_copy(step, me).start()
    for step in range(1, group):
        q_copy(step, me).wait_send()
    for step in range(1, group):
        s_copy(step, lax.rem(me + step, group)).wait_recv()
    out_ref[...] = sall_ref[...].reshape(n_rows, 128)
    for step in range(1, group):
        s_copy(step, me).wait_send()


def finish(sizes, temp_ref, scores_ref, rows_ref, mean_ref):
    outer, inner, per_dev = sizes[:3]
    n_rows = outer * inner * per_dev
    me = lax.axis_index('data2') * inner + lax.axis_index('data')
    lane = lax.broadcasted_iota(jnp.int32, (n_rows, 128), 1)
    doc = lax.broadcasted_iota(jnp.int32, (n_rows, 128), 0)
    logits = scores_ref[...] / temp_ref[0]
    top = jnp.max(logits, axis=0, keepdims=True)
    log_norm = top + jnp.log(jnp.sum(jnp.exp(logits - top), axis=0, keepdims=True))
    loss = log_norm - jnp.sum(jnp.where(doc == lane, logits, 0.0), axis=0, keepdims=True)
    loss = jnp.where(lane[:1] < n_rows, loss, 0.0)
    mean_ref[...] = jnp.sum(loss, axis=1, keepdims=True) / n_rows
    picked = jnp.where(lane[:8] == doc[:8] + me * per_dev, loss, 0.0)
    own = jnp.sum(picked, axis=1, keepdims=True)
    spread = jnp.where(lane[:8] == doc[:8], own, 0.0)
    rows_ref[...] = jnp.sum(spread, axis=0, keepdims=True)[:, :per_dev]


def solution(mesh):
    outer = mesh.shape['data2']
    inner = mesh.shape['data']
    group = outer * inner

    def device_fn(q_hidden, d_hidden, w_proj, q_mask, d_mask, value_a11):
        per_dev, q_len, hidden = q_hidden.shape
        d_len = d_hidden.shape[1]
        proj = w_proj.shape[1]
        sizes = (outer, inner, per_dev, q_len, d_len, hidden, proj)
        n_tok = per_dev * d_len
        n_rows = group * per_dev
        hbm_spec = pl.BlockSpec(memory_space=pltpu.HBM)
        vmem_spec = pl.BlockSpec(memory_space=pltpu.VMEM)
        scores = pl.pallas_call(
            functools.partial(kernel, sizes),
            out_shape=jax.ShapeDtypeStruct((n_rows, 128), jnp.float32),
            in_specs=[hbm_spec] * 5,
            out_specs=vmem_spec,
            scratch_shapes=[
                pltpu.VMEM((n_tok, hidden), jnp.bfloat16),
                pltpu.VMEM((per_dev * q_len, hidden), jnp.bfloat16),
                pltpu.VMEM((hidden, proj), jnp.bfloat16),
                pltpu.VMEM((proj, hidden), jnp.bfloat16),
                pltpu.VMEM((per_dev, q_len), jnp.int32),
                pltpu.VMEM((per_dev, d_len), jnp.int32),
                pltpu.VMEM((n_tok // STEP, proj + 16, STEP), jnp.bfloat16),
                pltpu.VMEM((group, per_dev * q_len, proj), jnp.bfloat16),
                pltpu.VMEM((per_dev, n_rows * q_len, 128), jnp.float32),
                pltpu.VMEM((group, per_dev, 128), jnp.float32),
                pltpu.SemaphoreType.DMA((4,)),
                pltpu.SemaphoreType.DMA((len(CHUNKS),)),
                pltpu.SemaphoreType.DMA((group,)),
                pltpu.SemaphoreType.DMA((group,)),
                pltpu.SemaphoreType.DMA((group,)),
                pltpu.SemaphoreType.DMA((group,)),
            ],
            compiler_params=pltpu.CompilerParams(
                collective_id=0, has_side_effects=True, vmem_limit_bytes=60 * 1024 * 1024),
            name='colbert_loss',
        )(q_hidden.reshape(per_dev * q_len, hidden), d_hidden.reshape(n_tok, hidden), w_proj, q_mask, d_mask)
        rows, mean = pl.pallas_call(
            functools.partial(finish, sizes),
            out_shape=(jax.ShapeDtypeStruct((1, per_dev), jnp.float32), jax.ShapeDtypeStruct((1, 1), jnp.float32)),
            in_specs=[pl.BlockSpec(memory_space=pltpu.SMEM), vmem_spec],
            out_specs=(vmem_spec, vmem_spec),
            name='loss_rows',
        )(value_a11.reshape(1), scores)
        return rows.reshape(per_dev), mean.reshape(1)

    return jax.shard_map(
        device_fn,
        mesh=mesh,
        in_specs=(P(ROW_AXES), P(ROW_AXES), P(), P(ROW_AXES), P(ROW_AXES), P()),
        out_specs=(P(ROW_AXES), P('replica')),
        check_vma=False,
    )
```

```python
import functools

import jax
import jax.numpy as jnp
from jax import lax
from jax.experimental import pallas as pl
from jax.experimental.pallas import tpu as pltpu
from jax.sharding import PartitionSpec as P

NORM_EPS = 1e-6
ROW_AXES = ('replica', 'data2', 'data')
TILE = 256
STEP = 2 * TILE
CHUNKS = (2, 3, 4, 4, 6, 8, 5)
LEAD = 9
EARLY = 12
RESERVE = 5
PIECE = 256
MASKED = -1e30
MESH = pl.DeviceIdType.MESH


def kernel(sizes, q_hbm, d_hbm, w_hbm, qm_hbm, dm_hbm, out_ref,
           h_ref, q_ref, w_ref, wt_ref, qm_ref, dm_ref, y_ref, et_ref, qall_ref, best_ref, sall_ref,
           in_sem, h_sem, q_send, q_recv, s_send, s_recv):
    outer, inner, per_dev, q_len, d_len, hidden, proj = sizes
    group = outer * inner
    n_rows = group * per_dev
    n_steps = per_dev * d_len // STEP
    doc_steps = d_len // STEP
    k_tiles = hidden // TILE
    q_rows = per_dev * q_len
    per_piece = PIECE // q_rows
    d2 = lax.axis_index('data2')
    d1 = lax.axis_index('data')
    me = d2 * inner + d1

    def partner(r):
        y = lax.rem(d2 + r // 4, 2)
        x = lax.rem(d1 // 2 + r // 2 % 2, 2)
        core = lax.rem(d1 + r % 2, 2)
        return y, x * 2 + core

    def target(r):
        y, x = partner(r)
        return {'data2': y, 'data': x}

    small = [pltpu.make_async_copy(src, dst, in_sem.at[i]) for i, (src, dst) in enumerate((
        (w_hbm, w_ref), (q_hbm, q_ref), (qm_hbm, qm_ref), (dm_hbm, dm_ref)))]
    for copy in small:
        copy.start()

    barrier = pltpu.get_barrier_semaphore()
    for r in range(1, group):
        pl.semaphore_signal(barrier, inc=1, device_id=target(r), device_id_type=MESH)

    starts = [sum(CHUNKS[:i]) for i in range(len(CHUNKS))]

    def h_copy(chunk):
        rows = pl.ds(starts[chunk] * STEP, CHUNKS[chunk] * STEP)
        return pltpu.make_async_copy(d_hbm.at[rows], h_ref.at[rows], h_sem.at[chunk])

    for chunk in range(len(CHUNKS)):
        h_copy(chunk).start(priority=1)

    for copy in small[:3]:
        copy.wait()
    y = jnp.dot(q_ref[...], w_ref[...], preferred_element_type=jnp.float32)
    unit = y * lax.rsqrt(jnp.sum(y * y, axis=1, keepdims=True) + NORM_EPS)
    eye = (lax.broadcasted_iota(jnp.int32, (q_len, q_len), 0)
           == lax.broadcasted_iota(jnp.int32, (q_len, q_len), 1))
    for i in range(per_dev):
        keep = jnp.sum(jnp.where(eye, qm_ref[i:i + 1, :], 0), axis=1, keepdims=True)
        rows = jnp.where(keep > 0, unit[i * q_len:(i + 1) * q_len], 0.0)
        qall_ref[0, i * q_len:(i + 1) * q_len, :] = rows.astype(jnp.bfloat16)

    pl.semaphore_wait(barrier, group - 1)

    def q_copy(r):
        return pltpu.make_async_remote_copy(
            src_ref=qall_ref.at[0], dst_ref=qall_ref.at[r], send_sem=q_send, recv_sem=q_recv.at[r // per_piece],
            device_id=target(r), device_id_type=MESH)

    def s_copy(r, slot):
        return pltpu.make_async_remote_copy(
            src_ref=sall_ref.at[slot], dst_ref=sall_ref.at[slot], send_sem=s_send, recv_sem=s_recv,
            device_id=target(r), device_id_type=MESH)

    for r in range(1, group):
        q_copy(r).start()
    wt_ref[...] = jnp.transpose(w_ref[...], (1, 0))
    small[3].wait()

    def doc_row(doc):
        lane = lax.broadcasted_iota(jnp.int32, (q_rows, 128), 1)
        query = lax.broadcasted_iota(jnp.int32, (q_rows, 128), 0) // q_len
        total = jnp.zeros((q_rows, 128), jnp.float32)
        for r in range(group):
            m = jnp.max(best_ref[doc, r * q_rows:(r + 1) * q_rows, :], axis=1, keepdims=True)
            py, px = partner(r)
            total = jnp.where(lane - (py * inner + px) * per_dev == query, m, total)
        return jnp.sum(total, axis=0, keepdims=True)

    ones_col = jnp.where(lax.broadcasted_iota(jnp.int32, (PIECE, 128), 1) == 0, 1.0, 0.0).astype(jnp.bfloat16)
    top_row = lax.broadcasted_iota(jnp.int32, (16, STEP), 0) == 0
    zeros = jnp.zeros((TILE - proj - 16, STEP), jnp.bfloat16)

    def project(step, k):
        h = h_ref[step * STEP:(step + 1) * STEP, k * TILE:(k + 1) * TILE]
        y = lax.dot_general(wt_ref[:, k * TILE:(k + 1) * TILE], h, (((1,), (1,)), ((), ())),
                            preferred_element_type=jnp.float32)
        slot = step % 2 + me // group
        if k:
            y = y_ref[slot] + y
        if k < k_tiles - 1:
            y_ref[slot] = y
            return
        inv = lax.rsqrt(jnp.sum(y * y, axis=0, keepdims=True) + NORM_EPS)
        et_ref[step, :proj, :] = (y * inv).astype(jnp.bfloat16)
        doc = step * STEP // d_len
        col = step * STEP % d_len
        valid = dm_ref[doc:doc + 1, col:col + STEP] > 0
        bias = jnp.where(top_row, jnp.where(valid, 0.0, MASKED), 0.0)
        et_ref[step, proj:, :] = bias.astype(jnp.bfloat16)

    def score(step, piece):
        doc = step // doc_steps
        q = qall_ref[piece * per_piece:(piece + 1) * per_piece].reshape(PIECE, proj)
        lhs = jnp.concatenate([q, ones_col], axis=1)
        rhs = jnp.concatenate([et_ref[step], zeros], axis=0)
        s = jnp.dot(lhs, rhs, preferred_element_type=jnp.float32)
        m = jnp.maximum(jnp.maximum(s[:, :128], s[:, 128:256]), jnp.maximum(s[:, 256:384], s[:, 384:]))
        rows = pl.ds(piece * PIECE, PIECE)
        if step % doc_steps:
            m = jnp.maximum(m, best_ref[doc, rows, :])
        best_ref[doc, rows, :] = m
        if step == doc_steps - 1 and piece == 1:
            sall_ref[me, 0:1, :] = doc_row(0)

    def receive(piece):
        landed = qall_ref.at[max(1, piece * per_piece):(piece + 1) * per_piece]
        pltpu.make_async_copy(landed, landed, q_recv.at[piece]).wait()

    projects = [(step, k) for step in range(n_steps) for k in range(k_tiles)]
    scores = ([(step, 0) for step in range(EARLY)] + [(step, 1) for step in range(EARLY)]
              + [(step, piece) for step in range(EARLY, n_steps) for piece in range(2)])

    pending = list(starts)

    def arrive():
        if projects and projects[0][1] == 0 and projects[0][0] in pending:
            pending.remove(projects[0][0])
            h_copy(starts.index(projects[0][0])).wait()

    for _ in range(LEAD * k_tiles):
        arrive()
        project(*projects.pop(0))
    spare = len(projects) - (len(scores) - RESERVE)
    for i, item in enumerate(scores):
        if i in (0, EARLY):
            receive(i // EARLY)
        arrive()
        score(*item)
        for _ in range(2 if i < spare else 1):
            if projects:
                arrive()
                project(*projects.pop(0))

    sall_ref[me, 1:2, :] = doc_row(1)

    for r in range(1, group):
        s_copy(r, me).start()
    others = qall_ref.at[1:]
    pltpu.make_async_copy(others, others, q_send).wait()
    others = sall_ref.at[1:]
    pltpu.make_async_copy(others, others, s_recv).wait()
    out_ref[...] = sall_ref[...].reshape(n_rows, 128)
    pltpu.make_async_copy(others, others, s_send).wait()


def finish(sizes, temp_ref, scores_ref, rows_ref, mean_ref):
    outer, inner, per_dev = sizes[:3]
    n_rows = outer * inner * per_dev
    me = lax.axis_index('data2') * inner + lax.axis_index('data')
    lane = lax.broadcasted_iota(jnp.int32, (n_rows, 128), 1)
    doc = lax.broadcasted_iota(jnp.int32, (n_rows, 128), 0)
    logits = scores_ref[...] / temp_ref[0]
    top = jnp.max(logits, axis=0, keepdims=True)
    log_norm = top + jnp.log(jnp.sum(jnp.exp(logits - top), axis=0, keepdims=True))
    loss = log_norm - jnp.sum(jnp.where(doc == lane, logits, 0.0), axis=0, keepdims=True)
    loss = jnp.where(lane[:1] < n_rows, loss, 0.0)
    mean_ref[...] = jnp.sum(loss, axis=1, keepdims=True) / n_rows
    picked = jnp.where(lane[:8] == doc[:8] + me * per_dev, loss, 0.0)
    own = jnp.sum(picked, axis=1, keepdims=True)
    spread = jnp.where(lane[:8] == doc[:8], own, 0.0)
    rows_ref[...] = jnp.sum(spread, axis=0, keepdims=True)[:, :per_dev]


def solution(mesh):
    outer = mesh.shape['data2']
    inner = mesh.shape['data']
    group = outer * inner

    def device_fn(q_hidden, d_hidden, w_proj, q_mask, d_mask, value_a11):
        per_dev, q_len, hidden = q_hidden.shape
        d_len = d_hidden.shape[1]
        proj = w_proj.shape[1]
        sizes = (outer, inner, per_dev, q_len, d_len, hidden, proj)
        n_tok = per_dev * d_len
        n_rows = group * per_dev
        hbm_spec = pl.BlockSpec(memory_space=pltpu.HBM)
        vmem_spec = pl.BlockSpec(memory_space=pltpu.VMEM)
        scores = pl.pallas_call(
            functools.partial(kernel, sizes),
            out_shape=pltpu.VMEM((n_rows, 128), jnp.float32),
            in_specs=[hbm_spec] * 5,
            out_specs=vmem_spec,
            scratch_shapes=[
                pltpu.VMEM((n_tok, hidden), jnp.bfloat16),
                pltpu.VMEM((per_dev * q_len, hidden), jnp.bfloat16),
                pltpu.VMEM((hidden, proj), jnp.bfloat16),
                pltpu.VMEM((proj, hidden), jnp.bfloat16),
                pltpu.VMEM((per_dev, q_len), jnp.int32),
                pltpu.VMEM((per_dev, d_len), jnp.int32),
                pltpu.VMEM((2, proj, STEP), jnp.float32),
                pltpu.VMEM((n_tok // STEP, proj + 16, STEP), jnp.bfloat16),
                pltpu.VMEM((group, per_dev * q_len, proj), jnp.bfloat16),
                pltpu.VMEM((per_dev, n_rows * q_len, 128), jnp.float32),
                pltpu.VMEM((group, per_dev, 128), jnp.float32),
                pltpu.SemaphoreType.DMA((4,)),
                pltpu.SemaphoreType.DMA((len(CHUNKS),)),
                pltpu.SemaphoreType.DMA(()),
                pltpu.SemaphoreType.DMA((2,)),
                pltpu.SemaphoreType.DMA(()),
                pltpu.SemaphoreType.DMA(()),
            ],
            compiler_params=pltpu.CompilerParams(
                collective_id=0, has_side_effects=True, vmem_limit_bytes=60 * 1024 * 1024),
            name='colbert_scores',
        )(q_hidden.reshape(per_dev * q_len, hidden), d_hidden.reshape(n_tok, hidden), w_proj, q_mask, d_mask)
        rows, mean = pl.pallas_call(
            functools.partial(finish, sizes),
            out_shape=(jax.ShapeDtypeStruct((1, per_dev), jnp.float32), jax.ShapeDtypeStruct((1, 1), jnp.float32)),
            in_specs=[pl.BlockSpec(memory_space=pltpu.SMEM), vmem_spec],
            out_specs=(vmem_spec, vmem_spec),
            name='loss_rows',
        )(value_a11.reshape(1), pltpu.with_memory_space_constraint(scores, pltpu.VMEM))
        return rows.reshape(per_dev), mean.reshape(1)

    return jax.shard_map(
        device_fn,
        mesh=mesh,
        in_specs=(P(ROW_AXES), P(ROW_AXES), P(), P(ROW_AXES), P(ROW_AXES), P()),
        out_specs=(P(ROW_AXES), P('replica')),
        check_vma=False,
    )
```

```python
import functools

import jax
import jax.numpy as jnp
from jax import lax
from jax.experimental import pallas as pl
from jax.experimental.pallas import tpu as pltpu
from jax.sharding import PartitionSpec as P

NORM_EPS = 1e-6
ROW_AXES = ('replica', 'data2', 'data')
TILE = 256
STEP = 2 * TILE
CHUNKS = (2,3,6,5,7,9)
LEAD = 5
EARLY = 9
RESERVE = 5
TURN = 1
PIECE = 256
MASKED = -1e30
MESH = pl.DeviceIdType.MESH


def kernel(sizes, q_hbm, d_hbm, w_hbm, qm_hbm, dm_hbm, out_ref,
           h_ref, q_ref, w_ref, wt_ref, qm_ref, dm_ref, y_ref, ht_ref, et_ref, qall_ref, best_ref, sall_ref,
           in_sem, h_sem, q_send, q_recv, s_send, s_recv):
    outer, inner, per_dev, q_len, d_len, hidden, proj = sizes
    group = outer * inner
    n_rows = group * per_dev
    n_steps = per_dev * d_len // STEP
    doc_steps = d_len // STEP
    k_tiles = hidden // TILE
    q_rows = per_dev * q_len
    per_piece = PIECE // q_rows
    d2 = lax.axis_index('data2')
    d1 = lax.axis_index('data')
    me = d2 * inner + d1

    def partner(r):
        y = lax.rem(d2 + r // 4, 2)
        x = lax.rem(d1 // 2 + r // 2 % 2, 2)
        core = lax.rem(d1 + r % 2, 2)
        return y, x * 2 + core

    def target(r):
        y, x = partner(r)
        return {'data2': y, 'data': x}

    small = [pltpu.make_async_copy(src, dst, in_sem.at[i]) for i, (src, dst) in enumerate((
        (w_hbm, w_ref), (q_hbm, q_ref), (qm_hbm, qm_ref), (dm_hbm, dm_ref)))]
    small[0].start()
    small[1].start()

    starts = [sum(CHUNKS[:i]) for i in range(len(CHUNKS))]

    def h_copy(chunk):
        rows = pl.ds(starts[chunk] * STEP, CHUNKS[chunk] * STEP)
        return pltpu.make_async_copy(d_hbm.at[rows], h_ref.at[rows], h_sem.at[chunk])

    for chunk in range(len(CHUNKS)):
        h_copy(chunk).start(priority=1)
    small[2].start()
    small[3].start()

    barrier = pltpu.get_barrier_semaphore()
    for r in range(1, group):
        pl.semaphore_signal(barrier, inc=1, device_id=target(r), device_id_type=MESH)

    for copy in small[:3]:
        copy.wait()
    y = jnp.dot(q_ref[...], w_ref[...], preferred_element_type=jnp.float32)
    unit = y * lax.rsqrt(jnp.sum(y * y, axis=1, keepdims=True) + NORM_EPS)
    eye = (lax.broadcasted_iota(jnp.int32, (q_len, q_len), 0)
           == lax.broadcasted_iota(jnp.int32, (q_len, q_len), 1))
    for i in range(per_dev):
        keep = jnp.sum(jnp.where(eye, qm_ref[i:i + 1, :], 0), axis=1, keepdims=True)
        rows = jnp.where(keep > 0, unit[i * q_len:(i + 1) * q_len], 0.0)
        qall_ref[0, i * q_len:(i + 1) * q_len, :] = rows.astype(jnp.bfloat16)

    pl.semaphore_wait(barrier, group - 1)

    def q_copy(r):
        return pltpu.make_async_remote_copy(
            src_ref=qall_ref.at[0], dst_ref=qall_ref.at[r], send_sem=q_send, recv_sem=q_recv.at[r // per_piece],
            device_id=target(r), device_id_type=MESH)

    def s_copy(r, slot):
        return pltpu.make_async_remote_copy(
            src_ref=sall_ref.at[slot], dst_ref=sall_ref.at[slot], send_sem=s_send, recv_sem=s_recv,
            device_id=target(r), device_id_type=MESH)

    for r in range(1, group):
        q_copy(r).start()
    wt_ref[...] = jnp.transpose(w_ref[...], (1, 0))
    small[3].wait()

    def doc_row(doc):
        lane = lax.broadcasted_iota(jnp.int32, (q_rows, 128), 1)
        query = lax.broadcasted_iota(jnp.int32, (q_rows, 128), 0) // q_len
        total = jnp.zeros((q_rows, 128), jnp.float32)
        for r in range(group):
            m = jnp.max(best_ref[doc, r * q_rows:(r + 1) * q_rows, :], axis=1, keepdims=True)
            py, px = partner(r)
            total = jnp.where(lane - (py * inner + px) * per_dev == query, m, total)
        return jnp.sum(total, axis=0, keepdims=True)

    ones_col = jnp.where(lax.broadcasted_iota(jnp.int32, (PIECE, 128), 1) == 0, 1.0, 0.0).astype(jnp.bfloat16)
    top_row = lax.broadcasted_iota(jnp.int32, (16, STEP), 0) == 0
    zeros = jnp.zeros((TILE - proj - 16, STEP), jnp.bfloat16)

    turned = []

    def turn_tile(step, k):
        slot = len(turned) % 2 + me // group
        turned.append((step, k, slot))
        ht_ref[slot] = jnp.transpose(h_ref[step * STEP:(step + 1) * STEP, k * TILE:(k + 1) * TILE], (1, 0))

    def project(step, k):
        h = h_ref[step * STEP:(step + 1) * STEP, k * TILE:(k + 1) * TILE]
        w = wt_ref[:, k * TILE:(k + 1) * TILE]
        if turned and turned[-1][:2] == (step, k):
            y = jnp.dot(w, ht_ref[turned[-1][2]], preferred_element_type=jnp.float32)
        else:
            y = lax.dot_general(w, h, (((1,), (1,)), ((), ())), preferred_element_type=jnp.float32)
        slot = step % 2 + me // group
        if k:
            y = y_ref[slot] + y
        if k < k_tiles - 1:
            y_ref[slot] = y
            return
        inv = lax.rsqrt(jnp.sum(y * y, axis=0, keepdims=True) + NORM_EPS)
        et_ref[step, :proj, :] = (y * inv).astype(jnp.bfloat16)
        doc = step * STEP // d_len
        col = step * STEP % d_len
        valid = dm_ref[doc:doc + 1, col:col + STEP] > 0
        bias = jnp.where(top_row, jnp.where(valid, 0.0, MASKED), 0.0)
        et_ref[step, proj:, :] = bias.astype(jnp.bfloat16)

    def score(step, piece):
        doc = step // doc_steps
        q = qall_ref[piece * per_piece:(piece + 1) * per_piece].reshape(PIECE, proj)
        lhs = jnp.concatenate([q, ones_col], axis=1)
        rhs = jnp.concatenate([et_ref[step], zeros], axis=0)
        s = jnp.dot(lhs, rhs, preferred_element_type=jnp.float32)
        m = jnp.maximum(jnp.maximum(s[:, :128], s[:, 128:256]), jnp.maximum(s[:, 256:384], s[:, 384:]))
        rows = pl.ds(piece * PIECE, PIECE)
        if step % doc_steps:
            m = jnp.maximum(m, best_ref[doc, rows, :])
        best_ref[doc, rows, :] = m
        if step == doc_steps - 1 and piece == 1:
            sall_ref[me, 0:1, :] = doc_row(0)

    def receive(piece):
        landed = qall_ref.at[max(1, piece * per_piece):(piece + 1) * per_piece]
        pltpu.make_async_copy(landed, landed, q_recv.at[piece]).wait()

    projects = [(step, k) for step in range(n_steps) for k in range(k_tiles)]
    scores = ([(step, 0) for step in range(EARLY)] + [(step, 1) for step in range(EARLY)]
              + [(step, piece) for step in range(EARLY, n_steps) for piece in range(2)])

    pending = list(starts)

    def arrive(count=1):
        for item in projects[:count]:
            if item[1] == 0 and item[0] in pending:
                pending.remove(item[0])
                h_copy(starts.index(item[0])).wait()

    lead = LEAD * k_tiles
    while lead > 0:
        pair = min(2, lead)
        arrive(pair)
        if pair == 2 and TURN:
            turn_tile(*projects[1])
        for _ in range(pair):
            project(*projects.pop(0))
        lead -= pair
    spare = len(projects) - (len(scores) - RESERVE)
    for i, item in enumerate(scores):
        count = 2 if i < spare else 1
        if i in (0, EARLY):
            receive(i // EARLY)
        arrive(count)
        if count == 2 and len(projects) > 1:
            turn_tile(*projects[1])
        score(*item)
        for _ in range(count):
            if projects:
                project(*projects.pop(0))

    sall_ref[me, 1:2, :] = doc_row(1)

    for r in range(1, group):
        s_copy(r, me).start()
    others = qall_ref.at[1:]
    pltpu.make_async_copy(others, others, q_send).wait()
    others = sall_ref.at[1:]
    pltpu.make_async_copy(others, others, s_recv).wait()
    out_ref[...] = sall_ref[...].reshape(n_rows, 128)
    pltpu.make_async_copy(others, others, s_send).wait()


def finish(sizes, temp_ref, scores_ref, rows_ref, mean_ref):
    outer, inner, per_dev = sizes[:3]
    n_rows = outer * inner * per_dev
    me = lax.axis_index('data2') * inner + lax.axis_index('data')
    lane = lax.broadcasted_iota(jnp.int32, (n_rows, 128), 1)
    doc = lax.broadcasted_iota(jnp.int32, (n_rows, 128), 0)
    logits = scores_ref[...] / temp_ref[0]
    top = jnp.max(logits, axis=0, keepdims=True)
    log_norm = top + jnp.log(jnp.sum(jnp.exp(logits - top), axis=0, keepdims=True))
    loss = log_norm - jnp.sum(jnp.where(doc == lane, logits, 0.0), axis=0, keepdims=True)
    loss = jnp.where(lane[:1] < n_rows, loss, 0.0)
    mean_ref[...] = jnp.sum(loss, axis=1, keepdims=True) / n_rows
    picked = jnp.where(lane[:8] == doc[:8] + me * per_dev, loss, 0.0)
    own = jnp.sum(picked, axis=1, keepdims=True)
    spread = jnp.where(lane[:8] == doc[:8], own, 0.0)
    rows_ref[...] = jnp.sum(spread, axis=0, keepdims=True)[:, :per_dev]


def solution(mesh):
    outer = mesh.shape['data2']
    inner = mesh.shape['data']
    group = outer * inner

    def device_fn(q_hidden, d_hidden, w_proj, q_mask, d_mask, value_a11):
        per_dev, q_len, hidden = q_hidden.shape
        d_len = d_hidden.shape[1]
        proj = w_proj.shape[1]
        sizes = (outer, inner, per_dev, q_len, d_len, hidden, proj)
        n_tok = per_dev * d_len
        n_rows = group * per_dev
        hbm_spec = pl.BlockSpec(memory_space=pltpu.HBM)
        vmem_spec = pl.BlockSpec(memory_space=pltpu.VMEM)
        scores = pl.pallas_call(
            functools.partial(kernel, sizes),
            out_shape=pltpu.VMEM((n_rows, 128), jnp.float32),
            in_specs=[hbm_spec] * 5,
            out_specs=vmem_spec,
            scratch_shapes=[
                pltpu.VMEM((n_tok, hidden), jnp.bfloat16),
                pltpu.VMEM((per_dev * q_len, hidden), jnp.bfloat16),
                pltpu.VMEM((hidden, proj), jnp.bfloat16),
                pltpu.VMEM((proj, hidden), jnp.bfloat16),
                pltpu.VMEM((per_dev, q_len), jnp.int32),
                pltpu.VMEM((per_dev, d_len), jnp.int32),
                pltpu.VMEM((2, proj, STEP), jnp.float32),
                pltpu.VMEM((2, TILE, STEP), jnp.bfloat16),
                pltpu.VMEM((n_tok // STEP, proj + 16, STEP), jnp.bfloat16),
                pltpu.VMEM((group, per_dev * q_len, proj), jnp.bfloat16),
                pltpu.VMEM((per_dev, n_rows * q_len, 128), jnp.float32),
                pltpu.VMEM((group, per_dev, 128), jnp.float32),
                pltpu.SemaphoreType.DMA((4,)),
                pltpu.SemaphoreType.DMA((len(CHUNKS),)),
                pltpu.SemaphoreType.DMA(()),
                pltpu.SemaphoreType.DMA((2,)),
                pltpu.SemaphoreType.DMA(()),
                pltpu.SemaphoreType.DMA(()),
            ],
            compiler_params=pltpu.CompilerParams(
                collective_id=0, has_side_effects=True, vmem_limit_bytes=60 * 1024 * 1024),
            name='colbert_scores',
        )(q_hidden.reshape(per_dev * q_len, hidden), d_hidden.reshape(n_tok, hidden), w_proj, q_mask, d_mask)
        rows, mean = pl.pallas_call(
            functools.partial(finish, sizes),
            out_shape=(jax.ShapeDtypeStruct((1, per_dev), jnp.float32), jax.ShapeDtypeStruct((1, 1), jnp.float32)),
            in_specs=[pl.BlockSpec(memory_space=pltpu.SMEM), vmem_spec],
            out_specs=(vmem_spec, vmem_spec),
            name='loss_rows',
        )(value_a11.reshape(1), pltpu.with_memory_space_constraint(scores, pltpu.VMEM))
        return rows.reshape(per_dev), mean.reshape(1)

    return jax.shard_map(
        device_fn,
        mesh=mesh,
        in_specs=(P(ROW_AXES), P(ROW_AXES), P(), P(ROW_AXES), P(ROW_AXES), P()),
        out_specs=(P(ROW_AXES), P('replica')),
        check_vma=False,
    )
```

```python
import functools

import jax
import jax.numpy as jnp
from jax import lax
from jax.experimental import pallas as pl
from jax.experimental.pallas import tpu as pltpu
from jax.sharding import PartitionSpec as P

NORM_EPS = 1e-6
ROW_AXES = ('replica', 'data2', 'data')
TILE = 256
STEP = 2 * TILE
CHUNKS = (2, 3, 6, 5, 7, 9)
LEAD = 5
EARLY = 9
RESERVE = 5
TURN = 1
PIECE = 256
MASKED = -1e30
MESH = pl.DeviceIdType.MESH


def kernel(sizes, q_hbm, d_hbm, w_hbm, qm_hbm, dm_hbm, out_ref,
           h_ref, q_ref, w_ref, wt_ref, qm_ref, dm_ref, y_ref, ht_ref, et_ref, qall_ref, best_ref, sall_ref,
           in_sem, h_sem, q_send, q_recv, s_send, s_recv):
    outer, inner, per_dev, q_len, d_len, hidden, proj = sizes
    group = outer * inner
    n_rows = group * per_dev
    n_steps = per_dev * d_len // STEP
    doc_steps = d_len // STEP
    k_tiles = hidden // TILE
    q_rows = per_dev * q_len
    per_piece = PIECE // q_rows
    d2 = lax.axis_index('data2')
    d1 = lax.axis_index('data')
    me = d2 * inner + d1

    def partner(r):
        y = lax.rem(d2 + r // 4, 2)
        x = lax.rem(d1 // 2 + r // 2 % 2, 2)
        core = lax.rem(d1 + r % 2, 2)
        return y, x * 2 + core

    def place(r):
        x = partner(r)[1] // 2
        across, along = r // 2 % 2, r // 4
        return r % 2 + x * (2 * along + 4 * across) + (1 - x) * (2 * across + 4 * along)

    def holder(slot):
        first, second = slot // 2 % 2, slot // 4
        side = d1 // 2
        y = lax.rem(d2 + side * first + (1 - side) * second, 2)
        x = lax.rem(side + side * second + (1 - side) * first, 2)
        return y * inner + x * 2 + lax.rem(d1 + slot % 2, 2)

    def target(r):
        y, x = partner(r)
        return {'data2': y, 'data': x}

    small = [pltpu.make_async_copy(src, dst, in_sem.at[i]) for i, (src, dst) in enumerate((
        (w_hbm, w_ref), (q_hbm, q_ref), (qm_hbm, qm_ref), (dm_hbm, dm_ref)))]
    small[0].start()
    small[1].start()

    starts = [sum(CHUNKS[:i]) for i in range(len(CHUNKS))]

    def h_copy(chunk):
        rows = pl.ds(starts[chunk] * STEP, CHUNKS[chunk] * STEP)
        return pltpu.make_async_copy(d_hbm.at[rows], h_ref.at[rows], h_sem.at[chunk])

    for chunk in range(len(CHUNKS)):
        h_copy(chunk).start(priority=1)
    small[2].start()
    small[3].start()

    barrier = pltpu.get_barrier_semaphore()
    for r in range(1, group):
        pl.semaphore_signal(barrier, inc=1, device_id=target(r), device_id_type=MESH)

    for copy in small[:3]:
        copy.wait()
    y = jnp.dot(q_ref[...], w_ref[...], preferred_element_type=jnp.float32)
    unit = y * lax.rsqrt(jnp.sum(y * y, axis=1, keepdims=True) + NORM_EPS)
    eye = (lax.broadcasted_iota(jnp.int32, (q_len, q_len), 0)
           == lax.broadcasted_iota(jnp.int32, (q_len, q_len), 1))
    for i in range(per_dev):
        keep = jnp.sum(jnp.where(eye, qm_ref[i:i + 1, :], 0), axis=1, keepdims=True)
        rows = jnp.where(keep > 0, unit[i * q_len:(i + 1) * q_len], 0.0)
        qall_ref[0, i * q_len:(i + 1) * q_len, :] = rows.astype(jnp.bfloat16)

    pl.semaphore_wait(barrier, group - 1)

    def q_copy(r):
        return pltpu.make_async_remote_copy(
            src_ref=qall_ref.at[0], dst_ref=qall_ref.at[place(r)], send_sem=q_send,
            recv_sem=q_recv.at[place(r) // per_piece],
            device_id=target(r), device_id_type=MESH)

    def s_copy(r, slot):
        return pltpu.make_async_remote_copy(
            src_ref=sall_ref.at[slot], dst_ref=sall_ref.at[slot], send_sem=s_send, recv_sem=s_recv,
            device_id=target(r), device_id_type=MESH)

    for r in range(1, group):
        q_copy(r).start()
    wt_ref[...] = jnp.transpose(w_ref[...], (1, 0))
    small[3].wait()

    def doc_row(doc):
        lane = lax.broadcasted_iota(jnp.int32, (q_rows, 128), 1)
        query = lax.broadcasted_iota(jnp.int32, (q_rows, 128), 0) // q_len
        total = jnp.zeros((q_rows, 128), jnp.float32)
        for r in range(group):
            m = jnp.max(best_ref[doc, r * q_rows:(r + 1) * q_rows, :], axis=1, keepdims=True)
            total = jnp.where(lane - holder(r) * per_dev == query, m, total)
        return jnp.sum(total, axis=0, keepdims=True)

    ones_col = jnp.where(lax.broadcasted_iota(jnp.int32, (PIECE, 128), 1) == 0, 1.0, 0.0).astype(jnp.bfloat16)
    top_row = lax.broadcasted_iota(jnp.int32, (16, STEP), 0) == 0
    zeros = jnp.zeros((TILE - proj - 16, STEP), jnp.bfloat16)

    turned = []

    def turn_tile(step, k):
        slot = len(turned) % 2 + me // group
        turned.append((step, k, slot))
        ht_ref[slot] = jnp.transpose(h_ref[step * STEP:(step + 1) * STEP, k * TILE:(k + 1) * TILE], (1, 0))

    def project(step, k):
        h = h_ref[step * STEP:(step + 1) * STEP, k * TILE:(k + 1) * TILE]
        w = wt_ref[:, k * TILE:(k + 1) * TILE]
        if turned and turned[-1][:2] == (step, k):
            y = jnp.dot(w, ht_ref[turned[-1][2]], preferred_element_type=jnp.float32)
        else:
            y = lax.dot_general(w, h, (((1,), (1,)), ((), ())), preferred_element_type=jnp.float32)
        slot = step % 2 + me // group
        if k:
            y = y_ref[slot] + y
        if k < k_tiles - 1:
            y_ref[slot] = y
            return
        inv = lax.rsqrt(jnp.sum(y * y, axis=0, keepdims=True) + NORM_EPS)
        et_ref[step, :proj, :] = (y * inv).astype(jnp.bfloat16)
        doc = step * STEP // d_len
        col = step * STEP % d_len
        valid = dm_ref[doc:doc + 1, col:col + STEP] > 0
        bias = jnp.where(top_row, jnp.where(valid, 0.0, MASKED), 0.0)
        et_ref[step, proj:, :] = bias.astype(jnp.bfloat16)

    def score(step, piece):
        doc = step // doc_steps
        q = qall_ref[piece * per_piece:(piece + 1) * per_piece].reshape(PIECE, proj)
        lhs = jnp.concatenate([q, ones_col], axis=1)
        rhs = jnp.concatenate([et_ref[step], zeros], axis=0)
        s = jnp.dot(lhs, rhs, preferred_element_type=jnp.float32)
        m = jnp.maximum(jnp.maximum(s[:, :128], s[:, 128:256]), jnp.maximum(s[:, 256:384], s[:, 384:]))
        rows = pl.ds(piece * PIECE, PIECE)
        if step % doc_steps:
            m = jnp.maximum(m, best_ref[doc, rows, :])
        best_ref[doc, rows, :] = m
        if step == doc_steps - 1 and piece == 1:
            sall_ref[me, 0:1, :] = doc_row(0)

    def receive(piece):
        landed = qall_ref.at[max(1, piece * per_piece):(piece + 1) * per_piece]
        pltpu.make_async_copy(landed, landed, q_recv.at[piece]).wait()

    projects = [(step, k) for step in range(n_steps) for k in range(k_tiles)]
    scores = ([(step, 0) for step in range(EARLY)] + [(step, 1) for step in range(EARLY)]
              + [(step, piece) for step in range(EARLY, n_steps) for piece in range(2)])

    pending = list(starts)

    def arrive(count=1):
        for item in projects[:count]:
            if item[1] == 0 and item[0] in pending:
                pending.remove(item[0])
                h_copy(starts.index(item[0])).wait()

    lead = LEAD * k_tiles
    while lead > 0:
        pair = min(2, lead)
        arrive(pair)
        if pair == 2 and TURN:
            turn_tile(*projects[1])
        for _ in range(pair):
            project(*projects.pop(0))
        lead -= pair
    spare = len(projects) - (len(scores) - RESERVE)
    for i, item in enumerate(scores):
        count = 2 if i < spare else 1
        if i in (0, EARLY):
            receive(i // EARLY)
        arrive(count)
        if count == 2 and len(projects) > 1:
            turn_tile(*projects[1])
        score(*item)
        for _ in range(count):
            if projects:
                project(*projects.pop(0))

    sall_ref[me, 1:2, :] = doc_row(1)

    for r in range(1, group):
        s_copy(r, me).start()
    others = qall_ref.at[1:]
    pltpu.make_async_copy(others, others, q_send).wait()
    others = sall_ref.at[1:]
    pltpu.make_async_copy(others, others, s_recv).wait()
    out_ref[...] = sall_ref[...].reshape(n_rows, 128)
    pltpu.make_async_copy(others, others, s_send).wait()


def finish(sizes, temp_ref, scores_ref, rows_ref, mean_ref):
    outer, inner, per_dev = sizes[:3]
    n_rows = outer * inner * per_dev
    me = lax.axis_index('data2') * inner + lax.axis_index('data')
    lane = lax.broadcasted_iota(jnp.int32, (n_rows, 128), 1)
    doc = lax.broadcasted_iota(jnp.int32, (n_rows, 128), 0)
    logits = scores_ref[...] / temp_ref[0]
    top = jnp.max(logits, axis=0, keepdims=True)
    log_norm = top + jnp.log(jnp.sum(jnp.exp(logits - top), axis=0, keepdims=True))
    loss = log_norm - jnp.sum(jnp.where(doc == lane, logits, 0.0), axis=0, keepdims=True)
    loss = jnp.where(lane[:1] < n_rows, loss, 0.0)
    mean_ref[...] = jnp.sum(loss, axis=1, keepdims=True) / n_rows
    picked = jnp.where(lane[:8] == doc[:8] + me * per_dev, loss, 0.0)
    own = jnp.sum(picked, axis=1, keepdims=True)
    spread = jnp.where(lane[:8] == doc[:8], own, 0.0)
    rows_ref[...] = jnp.sum(spread, axis=0, keepdims=True)[:, :per_dev]


def solution(mesh):
    outer = mesh.shape['data2']
    inner = mesh.shape['data']
    group = outer * inner

    def device_fn(q_hidden, d_hidden, w_proj, q_mask, d_mask, value_a11):
        per_dev, q_len, hidden = q_hidden.shape
        d_len = d_hidden.shape[1]
        proj = w_proj.shape[1]
        sizes = (outer, inner, per_dev, q_len, d_len, hidden, proj)
        n_tok = per_dev * d_len
        n_rows = group * per_dev
        hbm_spec = pl.BlockSpec(memory_space=pltpu.HBM)
        vmem_spec = pl.BlockSpec(memory_space=pltpu.VMEM)
        scores = pl.pallas_call(
            functools.partial(kernel, sizes),
            out_shape=pltpu.VMEM((n_rows, 128), jnp.float32),
            in_specs=[hbm_spec] * 5,
            out_specs=vmem_spec,
            scratch_shapes=[
                pltpu.VMEM((n_tok, hidden), jnp.bfloat16),
                pltpu.VMEM((per_dev * q_len, hidden), jnp.bfloat16),
                pltpu.VMEM((hidden, proj), jnp.bfloat16),
                pltpu.VMEM((proj, hidden), jnp.bfloat16),
                pltpu.VMEM((per_dev, q_len), jnp.int32),
                pltpu.VMEM((per_dev, d_len), jnp.int32),
                pltpu.VMEM((2, proj, STEP), jnp.float32),
                pltpu.VMEM((2, TILE, STEP), jnp.bfloat16),
                pltpu.VMEM((n_tok // STEP, proj + 16, STEP), jnp.bfloat16),
                pltpu.VMEM((group, per_dev * q_len, proj), jnp.bfloat16),
                pltpu.VMEM((per_dev, n_rows * q_len, 128), jnp.float32),
                pltpu.VMEM((group, per_dev, 128), jnp.float32),
                pltpu.SemaphoreType.DMA((4,)),
                pltpu.SemaphoreType.DMA((len(CHUNKS),)),
                pltpu.SemaphoreType.DMA(()),
                pltpu.SemaphoreType.DMA((2,)),
                pltpu.SemaphoreType.DMA(()),
                pltpu.SemaphoreType.DMA(()),
            ],
            compiler_params=pltpu.CompilerParams(
                collective_id=0, has_side_effects=True, vmem_limit_bytes=60 * 1024 * 1024),
            name='colbert_scores',
        )(q_hidden.reshape(per_dev * q_len, hidden), d_hidden.reshape(n_tok, hidden), w_proj, q_mask, d_mask)
        rows, mean = pl.pallas_call(
            functools.partial(finish, sizes),
            out_shape=(jax.ShapeDtypeStruct((1, per_dev), jnp.float32), jax.ShapeDtypeStruct((1, 1), jnp.float32)),
            in_specs=[pl.BlockSpec(memory_space=pltpu.SMEM), vmem_spec],
            out_specs=(vmem_spec, vmem_spec),
            name='loss_rows',
        )(value_a11.reshape(1), pltpu.with_memory_space_constraint(scores, pltpu.VMEM))
        return rows.reshape(per_dev), mean.reshape(1)

    return jax.shard_map(
        device_fn,
        mesh=mesh,
        in_specs=(P(ROW_AXES), P(ROW_AXES), P(), P(ROW_AXES), P(ROW_AXES), P()),
        out_specs=(P(ROW_AXES), P('replica')),
        check_vma=False,
    )
```

```python
import functools

import jax
import jax.numpy as jnp
from jax import lax
from jax.experimental import pallas as pl
from jax.experimental.pallas import tpu as pltpu
from jax.sharding import PartitionSpec as P

NORM_EPS = 1e-6
ROW_AXES = ('replica', 'data2', 'data')
TILE = 256
STEP = 2 * TILE
CHUNKS = (2, 3, 6, 5, 7, 9)
LEAD = 5
EARLY = 9
RESERVE = 5
TURN = 1
PIECE = 256
MASKED = -1e30
MESH = pl.DeviceIdType.MESH


def kernel(sizes, q_hbm, d_hbm, w_hbm, qm_hbm, dm_hbm, out_ref,
           h_ref, q_ref, w_ref, wt_ref, qm_ref, dm_ref, y_ref, ht_ref, et_ref, qall_ref, best_ref, sall_ref,
           in_sem, h_sem, q_send, q_recv, s_send, s_recv):
    outer, inner, per_dev, q_len, d_len, hidden, proj = sizes
    group = outer * inner
    n_rows = group * per_dev
    n_steps = per_dev * d_len // STEP
    doc_steps = d_len // STEP
    k_tiles = hidden // TILE
    q_rows = per_dev * q_len
    per_piece = PIECE // q_rows
    d2 = lax.axis_index('data2')
    d1 = lax.axis_index('data')
    me = d2 * inner + d1

    def partner(r):
        y = lax.rem(d2 + r // 4, 2)
        x = lax.rem(d1 // 2 + r // 2 % 2, 2)
        core = lax.rem(d1 + r % 2, 2)
        return y, x * 2 + core

    def place(r):
        x = partner(r)[1] // 2
        across, along = r // 2 % 2, r // 4
        return r % 2 + x * (2 * along + 4 * across) + (1 - x) * (2 * across + 4 * along)

    def holder(slot):
        first, second = slot // 2 % 2, slot // 4
        side = d1 // 2
        y = lax.rem(d2 + side * first + (1 - side) * second, 2)
        x = lax.rem(side + side * second + (1 - side) * first, 2)
        return y * inner + x * 2 + lax.rem(d1 + slot % 2, 2)

    def target(r):
        y, x = partner(r)
        return {'data2': y, 'data': x}

    small = [pltpu.make_async_copy(src, dst, in_sem.at[i]) for i, (src, dst) in enumerate((
        (w_hbm, w_ref), (q_hbm, q_ref), (qm_hbm, qm_ref), (dm_hbm, dm_ref)))]
    small[0].start()
    small[1].start()

    starts = [sum(CHUNKS[:i]) for i in range(len(CHUNKS))]

    def h_copy(chunk):
        rows = pl.ds(starts[chunk] * STEP, CHUNKS[chunk] * STEP)
        return pltpu.make_async_copy(d_hbm.at[rows], h_ref.at[rows], h_sem.at[chunk])

    for chunk in range(len(CHUNKS)):
        h_copy(chunk).start(priority=1)
    small[2].start()
    small[3].start()

    barrier = pltpu.get_barrier_semaphore()
    for r in range(1, group):
        pl.semaphore_signal(barrier, inc=1, device_id=target(r), device_id_type=MESH)

    for copy in small:
        copy.wait()
    y = jnp.dot(q_ref[...], w_ref[...], preferred_element_type=jnp.float32)
    unit = y * lax.rsqrt(jnp.sum(y * y, axis=1, keepdims=True) + NORM_EPS)
    eye = (lax.broadcasted_iota(jnp.int32, (q_len, q_len), 0)
           == lax.broadcasted_iota(jnp.int32, (q_len, q_len), 1))
    for i in range(per_dev):
        keep = jnp.sum(jnp.where(eye, qm_ref[i:i + 1, :], 0), axis=1, keepdims=True)
        rows = jnp.where(keep > 0, unit[i * q_len:(i + 1) * q_len], 0.0)
        qall_ref[0, i * q_len:(i + 1) * q_len, :] = rows.astype(jnp.bfloat16)

    wt_ref[...] = jnp.transpose(w_ref[...], (1, 0))
    pl.semaphore_wait(barrier, group - 1)

    def q_copy(r):
        return pltpu.make_async_remote_copy(
            src_ref=qall_ref.at[0], dst_ref=qall_ref.at[place(r)], send_sem=q_send,
            recv_sem=q_recv.at[place(r) // per_piece],
            device_id=target(r), device_id_type=MESH)

    def s_copy(r, slot):
        return pltpu.make_async_remote_copy(
            src_ref=sall_ref.at[slot], dst_ref=sall_ref.at[slot], send_sem=s_send, recv_sem=s_recv,
            device_id=target(r), device_id_type=MESH)

    for r in (4, 2, 5, 3, 6, 7, 1):
        q_copy(r).start()

    def doc_row(doc):
        lane = lax.broadcasted_iota(jnp.int32, (q_rows, 128), 1)
        query = lax.broadcasted_iota(jnp.int32, (q_rows, 128), 0) // q_len
        total = jnp.zeros((q_rows, 128), jnp.float32)
        for r in range(group):
            m = jnp.max(best_ref[doc, r * q_rows:(r + 1) * q_rows, :], axis=1, keepdims=True)
            total = jnp.where(lane - holder(r) * per_dev == query, m, total)
        return jnp.sum(total, axis=0, keepdims=True)

    ones_col = jnp.where(lax.broadcasted_iota(jnp.int32, (PIECE, 128), 1) == 0, 1.0, 0.0).astype(jnp.bfloat16)
    top_row = lax.broadcasted_iota(jnp.int32, (16, STEP), 0) == 0
    zeros = jnp.zeros((TILE - proj - 16, STEP), jnp.bfloat16)

    turned = []

    def turn_tile(step, k):
        slot = len(turned) % 2 + me // group
        turned.append((step, k, slot))
        ht_ref[slot] = jnp.transpose(h_ref[step * STEP:(step + 1) * STEP, k * TILE:(k + 1) * TILE], (1, 0))

    def project(step, k):
        h = h_ref[step * STEP:(step + 1) * STEP, k * TILE:(k + 1) * TILE]
        w = wt_ref[:, k * TILE:(k + 1) * TILE]
        if turned and turned[-1][:2] == (step, k):
            y = jnp.dot(w, ht_ref[turned[-1][2]], preferred_element_type=jnp.float32)
        else:
            y = lax.dot_general(w, h, (((1,), (1,)), ((), ())), preferred_element_type=jnp.float32)
        slot = step % 2 + me // group
        if k:
            y = y_ref[slot] + y
        if k < k_tiles - 1:
            y_ref[slot] = y
            return
        inv = lax.rsqrt(jnp.sum(y * y, axis=0, keepdims=True) + NORM_EPS)
        et_ref[step, :proj, :] = (y * inv).astype(jnp.bfloat16)
        doc = step * STEP // d_len
        col = step * STEP % d_len
        valid = dm_ref[doc:doc + 1, col:col + STEP] > 0
        bias = jnp.where(top_row, jnp.where(valid, 0.0, MASKED), 0.0)
        et_ref[step, proj:, :] = bias.astype(jnp.bfloat16)

    def score(step, piece):
        doc = step // doc_steps
        q = qall_ref[piece * per_piece:(piece + 1) * per_piece].reshape(PIECE, proj)
        lhs = jnp.concatenate([q, ones_col], axis=1)
        rhs = jnp.concatenate([et_ref[step], zeros], axis=0)
        s = jnp.dot(lhs, rhs, preferred_element_type=jnp.float32)
        m = jnp.maximum(jnp.maximum(s[:, :128], s[:, 128:256]), jnp.maximum(s[:, 256:384], s[:, 384:]))
        rows = pl.ds(piece * PIECE, PIECE)
        if step % doc_steps:
            m = jnp.maximum(m, best_ref[doc, rows, :])
        best_ref[doc, rows, :] = m
        if step == doc_steps - 1 and piece == 1:
            sall_ref[me, 0:1, :] = doc_row(0)

    def receive(piece):
        landed = qall_ref.at[max(1, piece * per_piece):(piece + 1) * per_piece]
        pltpu.make_async_copy(landed, landed, q_recv.at[piece]).wait()

    projects = [(step, k) for step in range(n_steps) for k in range(k_tiles)]
    scores = ([(step, 0) for step in range(EARLY)] + [(step, 1) for step in range(EARLY)]
              + [(step, piece) for step in range(EARLY, n_steps) for piece in range(2)])

    pending = list(starts)

    def arrive(count=1):
        for item in projects[:count]:
            if item[1] == 0 and item[0] in pending:
                pending.remove(item[0])
                h_copy(starts.index(item[0])).wait()

    lead = LEAD * k_tiles
    while lead > 0:
        pair = min(2, lead)
        arrive(pair)
        if pair == 2 and TURN:
            turn_tile(*projects[1])
        for _ in range(pair):
            project(*projects.pop(0))
        lead -= pair
    spare = len(projects) - (len(scores) - RESERVE)
    for i, item in enumerate(scores):
        count = 2 if i < spare else 1
        if i in (0, EARLY):
            receive(i // EARLY)
        arrive(count)
        if count == 2 and len(projects) > 1:
            turn_tile(*projects[1])
        score(*item)
        for _ in range(count):
            if projects:
                project(*projects.pop(0))

    sall_ref[me, 1:2, :] = doc_row(1)

    for r in range(1, group):
        s_copy(r, me).start()
    others = qall_ref.at[1:]
    pltpu.make_async_copy(others, others, q_send).wait()
    others = sall_ref.at[1:]
    pltpu.make_async_copy(others, others, s_recv).wait()
    out_ref[...] = sall_ref[...].reshape(n_rows, 128)
    pltpu.make_async_copy(others, others, s_send).wait()


def finish(sizes, temp_ref, scores_ref, rows_ref, mean_ref):
    outer, inner, per_dev = sizes[:3]
    n_rows = outer * inner * per_dev
    me = lax.axis_index('data2') * inner + lax.axis_index('data')
    lane = lax.broadcasted_iota(jnp.int32, (n_rows, 128), 1)
    doc = lax.broadcasted_iota(jnp.int32, (n_rows, 128), 0)
    logits = scores_ref[...] / temp_ref[0]
    top = jnp.max(logits, axis=0, keepdims=True)
    log_norm = top + jnp.log(jnp.sum(jnp.exp(logits - top), axis=0, keepdims=True))
    loss = log_norm - jnp.sum(jnp.where(doc == lane, logits, 0.0), axis=0, keepdims=True)
    loss = jnp.where(lane[:1] < n_rows, loss, 0.0)
    mean_ref[...] = jnp.sum(loss, axis=1, keepdims=True) / n_rows
    picked = jnp.where(lane[:8] == doc[:8] + me * per_dev, loss, 0.0)
    own = jnp.sum(picked, axis=1, keepdims=True)
    spread = jnp.where(lane[:8] == doc[:8], own, 0.0)
    rows_ref[...] = jnp.sum(spread, axis=0, keepdims=True)[:, :per_dev]


def solution(mesh):
    outer = mesh.shape['data2']
    inner = mesh.shape['data']
    group = outer * inner

    def device_fn(q_hidden, d_hidden, w_proj, q_mask, d_mask, value_a11):
        per_dev, q_len, hidden = q_hidden.shape
        d_len = d_hidden.shape[1]
        proj = w_proj.shape[1]
        sizes = (outer, inner, per_dev, q_len, d_len, hidden, proj)
        n_tok = per_dev * d_len
        n_rows = group * per_dev
        hbm_spec = pl.BlockSpec(memory_space=pltpu.HBM)
        vmem_spec = pl.BlockSpec(memory_space=pltpu.VMEM)
        scores = pl.pallas_call(
            functools.partial(kernel, sizes),
            out_shape=pltpu.VMEM((n_rows, 128), jnp.float32),
            in_specs=[hbm_spec] * 5,
            out_specs=vmem_spec,
            scratch_shapes=[
                pltpu.VMEM((n_tok, hidden), jnp.bfloat16),
                pltpu.VMEM((per_dev * q_len, hidden), jnp.bfloat16),
                pltpu.VMEM((hidden, proj), jnp.bfloat16),
                pltpu.VMEM((proj, hidden), jnp.bfloat16),
                pltpu.VMEM((per_dev, q_len), jnp.int32),
                pltpu.VMEM((per_dev, d_len), jnp.int32),
                pltpu.VMEM((2, proj, STEP), jnp.float32),
                pltpu.VMEM((2, TILE, STEP), jnp.bfloat16),
                pltpu.VMEM((n_tok // STEP, proj + 16, STEP), jnp.bfloat16),
                pltpu.VMEM((group, per_dev * q_len, proj), jnp.bfloat16),
                pltpu.VMEM((per_dev, n_rows * q_len, 128), jnp.float32),
                pltpu.VMEM((group, per_dev, 128), jnp.float32),
                pltpu.SemaphoreType.DMA((4,)),
                pltpu.SemaphoreType.DMA((len(CHUNKS),)),
                pltpu.SemaphoreType.DMA(()),
                pltpu.SemaphoreType.DMA((2,)),
                pltpu.SemaphoreType.DMA(()),
                pltpu.SemaphoreType.DMA(()),
            ],
            compiler_params=pltpu.CompilerParams(
                collective_id=0, has_side_effects=True, vmem_limit_bytes=60 * 1024 * 1024),
            name='colbert_scores',
        )(q_hidden.reshape(per_dev * q_len, hidden), d_hidden.reshape(n_tok, hidden), w_proj, q_mask, d_mask)
        rows, mean = pl.pallas_call(
            functools.partial(finish, sizes),
            out_shape=(jax.ShapeDtypeStruct((1, per_dev), jnp.float32), jax.ShapeDtypeStruct((1, 1), jnp.float32)),
            in_specs=[pl.BlockSpec(memory_space=pltpu.SMEM), vmem_spec],
            out_specs=(vmem_spec, vmem_spec),
            name='loss_rows',
        )(value_a11.reshape(1), pltpu.with_memory_space_constraint(scores, pltpu.VMEM))
        return rows.reshape(per_dev), mean.reshape(1)

    return jax.shard_map(
        device_fn,
        mesh=mesh,
        in_specs=(P(ROW_AXES), P(ROW_AXES), P(), P(ROW_AXES), P(ROW_AXES), P()),
        out_specs=(P(ROW_AXES), P('replica')),
        check_vma=False,
    )
```
